8 devices in a mesh: dp: 2 (over z, y), tp: 4 (over x, core).
Axes of the slice: x: 2, y: 2, z: 1, core: 2. Of those that a mesh axis runs over, the one named last changes fastest.
Arguments:
- x_in: bfloat16 [2048, 3072], P(('dp', 'tp')), parts along dimension 0
- grad_y: bfloat16 [2048, 3072], P(('dp', 'tp')), parts along dimension 0
- norm_gain: float32 [2, 3072], replicated
- w_qkv: bfloat16 [2, 3072, 5120], P(None, None, 'tp')
- w_out: bfloat16 [2, 3072, 3072], P(None, 'tp')
- w_gate: bfloat16 [2, 3072, 8192], P(None, None, 'tp')
- w_up: bfloat16 [2, 3072, 8192], P(None, None, 'tp')
- w_down: bfloat16 [2, 8192, 3072], P(None, 'tp')
Outputs:
- output 1: bfloat16 [2048, 3072], P(('dp', 'tp')), parts along dimension 0
- output 2: float32 [4, 3072], P('dp'), parts along dimension 0
- output 3: bfloat16 [4, 3072, 5120], P('dp', None, 'tp'), parts along dimension 0
- output 4: bfloat16 [4, 3072, 3072], P('dp', 'tp'), parts along dimension 0
- output 5: bfloat16 [4, 3072, 8192], P('dp', None, 'tp'), parts along dimension 0
- output 6: bfloat16 [4, 3072, 8192], P('dp', None, 'tp'), parts along dimension 0
- output 7: bfloat16 [4, 8192, 3072], P('dp', 'tp'), parts along dimension 0
There are 2 independent parts. The reference program is written for one: setup_inputs(seed, part) draws one part's arguments, and reference() takes and returns one part's arrays. A program takes and returns all parts, laid end to end along the dimension named above; an argument that names none is the same for every part.
All inputs are finite; a program needn't handle non-finite values.
Results may differ from the reference program's by a relative error of at most 0.015981.
Values are sent between devices in bfloat16 or wider.
A program may use at most 1 GiB of HBM per device.

```python
import jax
import jax.numpy as jnp
from jax import lax

SEQ_LEN = 1024
D_MODEL = 3072
D_FF = 8192
HEADS = 24
KV_HEADS = 8
HEAD_DIM = 128
LAYERS = 2

GROUP_SIZE = HEADS // KV_HEADS
QKV_COLS = (HEADS + 2 * KV_HEADS) * HEAD_DIM
NORM_EPS = 1e-5
ROPE_BASE = 10000.0


def setup_inputs(seed: int = 0, part: int = 0) -> dict:
    data_keys = jax.random.split(jax.random.fold_in(jax.random.key(seed), part), 2)
    weight_keys = jax.random.split(jax.random.key(seed + 1), 6)
    x_in = jax.random.normal(data_keys[0], (SEQ_LEN, D_MODEL), jnp.float32)
    grad_y = jax.random.normal(data_keys[1], (SEQ_LEN, D_MODEL), jnp.float32)
    norm_gain = 1.0 + 0.3 * jax.random.normal(weight_keys[0], (LAYERS, D_MODEL), jnp.float32)
    w_qkv = jax.random.normal(weight_keys[1], (LAYERS, D_MODEL, QKV_COLS), jnp.float32) * D_MODEL ** -0.5
    w_out = jax.random.normal(weight_keys[2], (LAYERS, HEADS * HEAD_DIM, D_MODEL), jnp.float32) * (HEADS * HEAD_DIM) ** -0.5
    w_gate = jax.random.normal(weight_keys[3], (LAYERS, D_MODEL, D_FF), jnp.float32) * D_MODEL ** -0.5
    w_up = jax.random.normal(weight_keys[4], (LAYERS, D_MODEL, D_FF), jnp.float32) * D_MODEL ** -0.5
    w_down = jax.random.normal(weight_keys[5], (LAYERS, D_FF, D_MODEL), jnp.float32) * D_FF ** -0.5
    return {'x_in': x_in.astype(jnp.bfloat16), 'grad_y': grad_y.astype(jnp.bfloat16), 'norm_gain': norm_gain, 'w_qkv': w_qkv.astype(jnp.bfloat16), 'w_out': w_out.astype(jnp.bfloat16), 'w_gate': w_gate.astype(jnp.bfloat16), 'w_up': w_up.astype(jnp.bfloat16), 'w_down': w_down.astype(jnp.bfloat16)}


def rope_tables():
    half_dim = HEAD_DIM // 2
    freqs = ROPE_BASE ** (-2.0 * jnp.arange(half_dim, dtype=jnp.float32) / HEAD_DIM)
    angles = jnp.arange(SEQ_LEN, dtype=jnp.float32)[:, None] * freqs[None, :]
    return jnp.cos(angles)[:, None, None, :], jnp.sin(angles)[:, None, None, :]


def rotate(values, cos_tab, sin_tab):
    half_dim = values.shape[-1] // 2
    lower_half = values[..., :half_dim]
    upper_half = values[..., half_dim:]
    return jnp.concatenate([lower_half * cos_tab - upper_half * sin_tab, upper_half * cos_tab + lower_half * sin_tab], axis=-1)


def rms_scale(x_f32, gain_row):
    inv_rms = lax.rsqrt(jnp.mean(x_f32 * x_f32, axis=-1, keepdims=True) + NORM_EPS)
    return x_f32 * inv_rms * gain_row


def group_attention(operands):
    query, keys_rot, values_v = operands
    causal = jnp.arange(SEQ_LEN)[:, None] >= jnp.arange(SEQ_LEN)[None, :]
    scores = jnp.einsum('sgd,td->gst', query.astype(jnp.float32), keys_rot.astype(jnp.float32)) * HEAD_DIM ** -0.5
    attn_prob = jax.nn.softmax(jnp.where(causal, scores, -1e30), axis=-1).astype(jnp.bfloat16)
    return jnp.einsum('gst,td->sgd', attn_prob.astype(jnp.float32), values_v.astype(jnp.float32)).astype(jnp.bfloat16)


def decoder_block(x_cur, gain_row, w_qkv_l, w_out_l, w_gate_l, w_up_l, w_down_l, cos_tab, sin_tab):
    x_f32 = x_cur.astype(jnp.float32)
    normed = rms_scale(x_f32, gain_row).astype(jnp.bfloat16).astype(jnp.float32)
    qkv_all = jnp.dot(normed, w_qkv_l.astype(jnp.float32), preferred_element_type=jnp.float32).astype(jnp.bfloat16)
    qkv_all = qkv_all.reshape(SEQ_LEN, KV_HEADS, GROUP_SIZE + 2, HEAD_DIM)
    rotated = rotate(qkv_all[:, :, :GROUP_SIZE + 1].astype(jnp.float32), cos_tab, sin_tab).astype(jnp.bfloat16)
    operands = (jnp.moveaxis(rotated[:, :, :GROUP_SIZE], 1, 0), jnp.moveaxis(rotated[:, :, GROUP_SIZE], 1, 0), jnp.moveaxis(qkv_all[:, :, GROUP_SIZE + 1], 1, 0))
    attn_out = lax.map(jax.checkpoint(group_attention), operands)
    attn_out = jnp.moveaxis(attn_out, 0, 1).reshape(SEQ_LEN, HEADS * HEAD_DIM)
    gate_act = jnp.dot(normed, w_gate_l.astype(jnp.float32), preferred_element_type=jnp.float32).astype(jnp.bfloat16)
    up_act = jnp.dot(normed, w_up_l.astype(jnp.float32), preferred_element_type=jnp.float32).astype(jnp.bfloat16)
    hidden = (jax.nn.silu(gate_act.astype(jnp.float32)) * up_act.astype(jnp.float32)).astype(jnp.bfloat16)
    block_sum = x_f32 + jnp.dot(attn_out.astype(jnp.float32), w_out_l.astype(jnp.float32), preferred_element_type=jnp.float32) + jnp.dot(hidden.astype(jnp.float32), w_down_l.astype(jnp.float32), preferred_element_type=jnp.float32)
    return block_sum.astype(jnp.bfloat16)


def stack_forward(x_in, norm_gain, w_qkv, w_out, w_gate, w_up, w_down):
    cos_tab, sin_tab = rope_tables()

    def body(x_cur, layer_weights):
        gain_row, w_qkv_l, w_out_l, w_gate_l, w_up_l, w_down_l = layer_weights
        return decoder_block(x_cur, gain_row, w_qkv_l, w_out_l, w_gate_l, w_up_l, w_down_l, cos_tab, sin_tab), None

    return lax.scan(body, x_in, (norm_gain, w_qkv, w_out, w_gate, w_up, w_down))[0]


def reference(x_in, grad_y, norm_gain, w_qkv, w_out, w_gate, w_up, w_down):
    pullback = jax.vjp(stack_forward, x_in, norm_gain, w_qkv, w_out, w_gate, w_up, w_down)[1]
    grad_x, grad_gain, grad_qkv, grad_out, grad_gate, grad_up, grad_down = pullback(grad_y)
    return (grad_x, grad_gain, grad_qkv, grad_out, grad_gate, grad_up, grad_down)
```

```python
import functools

import jax
import jax.numpy as jnp
from jax import lax
from jax.experimental import pallas as pl
from jax.experimental.pallas import tpu as pltpu
from jax.sharding import PartitionSpec as P

HEAD_DIM = 128
NORM_EPS = 1e-5
ROPE_BASE = 10000.0
BF16 = jnp.bfloat16
F32 = jnp.float32
GROUP = 3
SCALE = HEAD_DIM ** -0.5
CORE_PAIRS = [(0, 1), (1, 0), (2, 3), (3, 2)]
CHIP_PAIRS = [(0, 2), (2, 0), (1, 3), (3, 1)]
VMEM_LIMIT = 60 << 20


def core_swap(values):
    return lax.ppermute(values, 'tp', CORE_PAIRS)


def chip_swap(values):
    return lax.ppermute(values, 'tp', CHIP_PAIRS)


def barrier(*values):
    return lax.optimization_barrier(values)


def rope_tables(seq_len):
    half_dim = HEAD_DIM // 2
    freqs = ROPE_BASE ** (-2.0 * jnp.arange(half_dim, dtype=F32) / HEAD_DIM)
    angles = jnp.arange(seq_len, dtype=F32)[:, None] * freqs[None, :]
    cos_tab, sin_tab = jnp.cos(angles), jnp.sin(angles)
    return jnp.concatenate([cos_tab, cos_tab], axis=1), jnp.concatenate([-sin_tab, sin_tab], axis=1)


def rms_scale(x_f32, gain_row):
    inv_rms = lax.rsqrt(jnp.mean(x_f32 * x_f32, axis=-1, keepdims=True) + NORM_EPS)
    return x_f32 * inv_rms * gain_row


def gated(gate_f32, up_f32):
    return jax.nn.silu(gate_f32) * up_f32


def dot(lhs, rhs):
    return jnp.dot(lhs, rhs, preferred_element_type=F32)


def dot_t(lhs, rhs):
    return lax.dot_general(lhs, rhs, (((1,), (1,)), ((), ())), preferred_element_type=F32)


def dot_lt(lhs, rhs):
    return lax.dot_general(lhs, rhs, (((0,), (0,)), ((), ())), preferred_element_type=F32)


def attn_fwd_kernel(base_ref, qn_ref, qf_ref, cos_ref, sin_ref, rq_ref, on_ref, of_ref, lse_ref, o_scr):
    rows = qn_ref.shape[0] // 2
    kcol, vcol = GROUP * HEAD_DIM, (GROUP + 1) * HEAD_DIM
    for k in range(4):
        src = qn_ref if k < 2 else qf_ref
        local = slice((k % 2) * rows, (k % 2 + 1) * rows)
        where = pl.ds(pl.multiple_of(base_ref[k] * rows, rows), rows)
        cos_tab, sin_tab = cos_ref[where, :], sin_ref[where, :]
        for h in range(GROUP + 1):
            cols = slice(h * HEAD_DIM, (h + 1) * HEAD_DIM)
            vals = src[local, cols].astype(F32)
            rq_ref[where, cols] = (vals * cos_tab + pltpu.roll(vals, HEAD_DIM // 2, 1) * sin_tab).astype(BF16)
        rq_ref[where, vcol:] = src[local, vcol:]
    causal = lax.broadcasted_iota(jnp.int32, (rows, rows), 0) >= lax.broadcasted_iota(jnp.int32, (rows, rows), 1)
    for i in range(4):
        width = (i + 1) * rows
        keys, vals = rq_ref[0:width, kcol:vcol], rq_ref[0:width, vcol:]
        for h in range(GROUP):
            query = rq_ref[i * rows:width, h * HEAD_DIM:(h + 1) * HEAD_DIM]
            scores = dot_t(query, keys) * SCALE
            diag = jnp.where(causal, scores[:, i * rows:], -1e30)
            scores = diag if i == 0 else jnp.concatenate([scores[:, :i * rows], diag], axis=1)
            row_max = jnp.max(scores, axis=1, keepdims=True)
            weights = jnp.exp(scores - row_max)
            total = jnp.sum(weights, axis=1, keepdims=True)
            prob = (weights * (1.0 / total)).astype(BF16)
            o_scr[i * rows:width, h * HEAD_DIM:(h + 1) * HEAD_DIM] = dot(prob, vals).astype(BF16)
            lse = jnp.broadcast_to(row_max + jnp.log(total), (rows, HEAD_DIM))
            lse_ref[0, h:h + 1, i * rows:width] = jnp.transpose(lse)[0:1, :]
    for k in range(4):
        dst = on_ref if k < 2 else of_ref
        dst[(k % 2) * rows:(k % 2 + 1) * rows, :] = o_scr[pl.ds(pl.multiple_of(base_ref[k] * rows, rows), rows), :]


def attn_fwd(base, qkv_n, qkv_f, cos_tab, sin_tab):
    half, width = cos_tab.shape[0] // 2, qkv_n.shape[1]
    cols = (GROUP + 2) * HEAD_DIM
    groups = width // cols
    seq_len = 2 * half
    smem = pl.BlockSpec(memory_space=pltpu.SMEM)
    tab = pl.BlockSpec((seq_len, HEAD_DIM), lambda j: (0, 0))
    half_in = pl.BlockSpec((half, cols), lambda j: (0, j))
    half_out = pl.BlockSpec((half, GROUP * HEAD_DIM), lambda j: (0, j))
    return pl.pallas_call(
        attn_fwd_kernel, grid=(groups,), name='attn_fwd',
        in_specs=[smem, half_in, half_in, tab, tab],
        out_specs=[pl.BlockSpec((seq_len, cols), lambda j: (0, j)), half_out, half_out, pl.BlockSpec((1, 8, seq_len), lambda j: (j, 0, 0))],
        out_shape=[jax.ShapeDtypeStruct((seq_len, width), BF16)] + [jax.ShapeDtypeStruct((half, groups * GROUP * HEAD_DIM), BF16)] * 2 + [jax.ShapeDtypeStruct((groups, 8, seq_len), F32)],
        scratch_shapes=[pltpu.VMEM((seq_len, GROUP * HEAD_DIM), BF16)],
        cost_estimate=pl.CostEstimate(flops=8 * 10 ** 9, bytes_accessed=8 * 10 ** 6, transcendentals=4 * 10 ** 6),
        compiler_params=pltpu.CompilerParams(vmem_limit_bytes=VMEM_LIMIT),
    )(base, qkv_n, qkv_f, cos_tab, sin_tab)


def attn_bwd_kernel(base_ref, rq_ref, lse_ref, dn_ref, df_ref, cos_ref, sin_ref, gn_ref, gf_ref, do_scr, dq_scr, dk_scr, dv_scr):
    rows = dn_ref.shape[0] // 2
    kcol, vcol = GROUP * HEAD_DIM, (GROUP + 1) * HEAD_DIM
    for k in range(4):
        src = dn_ref if k < 2 else df_ref
        do_scr[pl.ds(pl.multiple_of(base_ref[k] * rows, rows), rows), :] = src[(k % 2) * rows:(k % 2 + 1) * rows, :]
    dk_scr[...] = jnp.zeros_like(dk_scr)
    dv_scr[...] = jnp.zeros_like(dv_scr)
    causal = lax.broadcasted_iota(jnp.int32, (rows, rows), 1) >= lax.broadcasted_iota(jnp.int32, (rows, rows), 0)
    for i in range(4):
        width = (i + 1) * rows
        keys, vals = rq_ref[0:width, kcol:vcol], rq_ref[0:width, vcol:]
        for h in range(GROUP):
            cols = slice(h * HEAD_DIM, (h + 1) * HEAD_DIM)
            query, d_o = rq_ref[i * rows:width, cols], do_scr[i * rows:width, cols]
            scores = dot_t(keys, query) * SCALE
            diag = jnp.where(causal, scores[i * rows:, :], -1e30)
            scores = diag if i == 0 else jnp.concatenate([scores[:i * rows, :], diag], axis=0)
            prob = jnp.exp(scores - lse_ref[0, h:h + 1, i * rows:width])
            d_prob = dot_t(vals, d_o).astype(BF16).astype(F32)
            delta = jnp.sum(prob * d_prob, axis=0, keepdims=True)
            d_scores = (prob * (d_prob - delta) * SCALE).astype(BF16)
            dv_scr[0:width, :] += dot(prob.astype(BF16), d_o)
            dk_scr[0:width, :] += dot(d_scores, query)
            dq_scr[i * rows:width, cols] = dot_lt(d_scores, keys).astype(BF16)
    for k in range(4):
        dst = gn_ref if k < 2 else gf_ref
        local = slice((k % 2) * rows, (k % 2 + 1) * rows)
        where = pl.ds(pl.multiple_of(base_ref[k] * rows, rows), rows)
        cos_tab, sin_tab = cos_ref[where, :], sin_ref[where, :]
        for h in range(GROUP + 1):
            cols = slice(h * HEAD_DIM, (h + 1) * HEAD_DIM)
            vals = dq_scr[where, cols].astype(F32) if h < GROUP else dk_scr[where, :].astype(BF16).astype(F32)
            dst[local, cols] = (vals * cos_tab - pltpu.roll(vals, HEAD_DIM // 2, 1) * sin_tab).astype(BF16)
        dst[local, vcol:] = dv_scr[where, :].astype(BF16)


def attn_bwd(base, rot_qkv, lse, d_halves, cos_tab, sin_tab):
    seq_len, width = rot_qkv.shape
    half = seq_len // 2
    cols = (GROUP + 2) * HEAD_DIM
    groups = width // cols
    smem = pl.BlockSpec(memory_space=pltpu.SMEM)
    tab = pl.BlockSpec((seq_len, HEAD_DIM), lambda j: (0, 0))
    halves_in = [pl.BlockSpec((half, GROUP * HEAD_DIM), lambda j, r=r: (r, j)) for _, r in d_halves]
    half_out = pl.BlockSpec((half, cols), lambda j: (0, j))
    return pl.pallas_call(
        attn_bwd_kernel, grid=(groups,), name='attn_bwd',
        in_specs=[smem, pl.BlockSpec((seq_len, cols), lambda j: (0, j)), pl.BlockSpec((1, 8, seq_len), lambda j: (j, 0, 0)), *halves_in, tab, tab],
        out_specs=[half_out, half_out],
        out_shape=[jax.ShapeDtypeStruct((half, width), BF16)] * 2,
        scratch_shapes=[pltpu.VMEM((seq_len, GROUP * HEAD_DIM), BF16)] * 2 + [pltpu.VMEM((seq_len, HEAD_DIM), F32)] * 2,
        cost_estimate=pl.CostEstimate(flops=20 * 10 ** 9, bytes_accessed=8 * 10 ** 6, transcendentals=4 * 10 ** 6),
        compiler_params=pltpu.CompilerParams(vmem_limit_bytes=VMEM_LIMIT),
    )(base, rot_qkv, lse, d_halves[0][0], d_halves[1][0], cos_tab, sin_tab)


def wgrad_kernel(an_ref, af_ref, bn_ref, bf_ref, *rest):
    out_ref = rest[-1]
    out_ref[0] = (dot_lt(an_ref[...], bn_ref[...]) + dot_lt(af_ref[...], bf_ref[...])).astype(BF16)


def wgrad(half, lhs, rhs, layer_idx, n_layers, stacked, block_rows, name):
    m_dim, n_dim = lhs[0][0].shape[1], rhs[0][0].shape[1]
    in_specs = [pl.BlockSpec((half, block_rows), lambda m, r=r: (r, m)) for _, r in lhs]
    in_specs += [pl.BlockSpec((half, n_dim), lambda m, r=r: (r, 0)) for _, r in rhs]
    args = [arr for arr, _ in lhs + rhs]
    aliases = {}
    if stacked is not None:
        in_specs.append(pl.BlockSpec(memory_space=pl.ANY))
        args.append(stacked)
        aliases = {4: 0}
    return pl.pallas_call(
        wgrad_kernel, grid=(m_dim // block_rows,), name=name, in_specs=in_specs,
        out_specs=pl.BlockSpec((1, block_rows, n_dim), lambda m: (layer_idx, m, 0)),
        out_shape=jax.ShapeDtypeStruct((n_layers, m_dim, n_dim), BF16),
        input_output_aliases=aliases,
        cost_estimate=pl.CostEstimate(flops=4 * half * m_dim * n_dim, bytes_accessed=2 * (m_dim * n_dim + 2 * half * (m_dim + n_dim)), transcendentals=0),
        compiler_params=pltpu.CompilerParams(vmem_limit_bytes=VMEM_LIMIT),
    )(*args)


def fused_mm(name, rows, xs, ws, trans, layer, block, extras, epilogue, outs):
    n_dim = ws[0].shape[1] if trans else ws[0].shape[2]
    n_x, n_e = len(xs), len(extras)

    def kernel(*refs):
        accs = [(dot_t if trans else dot)(refs[i][...], refs[n_x + i][0]) for i in range(n_x)]
        results = epilogue(accs, [ref[...] for ref in refs[2 * n_x:2 * n_x + n_e]])
        for ref, val in zip(refs[2 * n_x + n_e:], results):
            ref[...] = val.astype(ref.dtype)

    in_specs = [pl.BlockSpec((rows, x.shape[1]), lambda n, r=r: (r, 0)) for x, r in xs]
    if trans:
        in_specs += [pl.BlockSpec((1, block, w.shape[2]), lambda n: (layer, n, 0)) for w in ws]
    else:
        in_specs += [pl.BlockSpec((1, w.shape[1], block), lambda n: (layer, 0, n)) for w in ws]
    in_specs += [pl.BlockSpec((rows, block), lambda n, r=r: (r, n)) for _, r in extras]
    depth = sum(x.shape[1] for x, _ in xs)
    return list(pl.pallas_call(
        kernel, grid=(n_dim // block,), name=name, in_specs=in_specs,
        out_specs=[pl.BlockSpec((r, block), lambda n: (0, n)) for r, _ in outs],
        out_shape=[jax.ShapeDtypeStruct((r, n_dim), dt) for r, dt in outs],
        cost_estimate=pl.CostEstimate(flops=2 * rows * depth * n_dim, bytes_accessed=2 * depth * (rows + n_dim) + 4 * rows * n_dim, transcendentals=0),
        compiler_params=pltpu.CompilerParams(vmem_limit_bytes=VMEM_LIMIT),
    )(*[x for x, _ in xs], *ws, *[e for e, _ in extras]))


def gate_up_epilogue(accs, extras):
    gate, up = accs[0].astype(BF16), accs[1].astype(BF16)
    return gate, up, gated(gate.astype(F32), up.astype(F32))


def gate_up_back_epilogue(accs, extras):
    gate, up = accs[0].astype(BF16).astype(F32), accs[1].astype(BF16).astype(F32)
    hidden, pull = jax.vjp(gated, gate, up)
    return (hidden,) + pull(extras[0].astype(F32))


def plain_epilogue(accs, extras):
    return accs


def split_sum_epilogue(accs, extras):
    total = sum(accs[1:], accs[0])
    rows = total.shape[0] // 2
    return total[:rows], total[rows:]


def mlp_back_epilogue(accs, extras):
    d_hid = accs[0].astype(BF16).astype(F32)
    gate, up = extras[0].astype(F32), extras[1].astype(F32)
    hidden, pull = jax.vjp(gated, gate, up)
    return (hidden,) + pull(d_hid)


def solution(mesh):
    row_spec = P(('dp', 'tp'), None)
    col_spec = P(None, None, 'tp')
    inner_spec = P(None, 'tp', None)

    def device_program(x_loc, dy_loc, norm_gain, w_qkv, w_out, w_gate, w_up, w_down):
        n_layers = w_qkv.shape[0]
        rows = x_loc.shape[0]
        half = 2 * rows
        rank = lax.axis_index('tp')
        base = jnp.bitwise_xor(jnp.arange(4, dtype=jnp.int32), rank.astype(jnp.int32))
        cos_tab, sin_tab = rope_tables(4 * rows)
        saved = []
        x_cur = x_loc

        def project(layer, u_half, d_hid):
            qkv = dot(u_half, w_qkv[layer]).astype(BF16)
            extras = [] if d_hid is None else [d_hid]
            epilogue = gate_up_epilogue if d_hid is None else gate_up_back_epilogue
            return [qkv] + fused_mm('gate_up', half, [(u_half, 0)] * 2, [w_gate, w_up], False, layer, 256, extras, epilogue, [(half, BF16)] * 3)

        def mlp_back(layer, n_rows, dy_half, gate_half, up_half):
            return fused_mm('mlp_back', n_rows, [(dy_half, 0)], [w_down], True, layer, 256, [(gate_half, 0), (up_half, 0)], mlp_back_epilogue, [(n_rows, BF16)] * 3)

        def wgrads(which, layer, u_halves, d_qkv, d_gate, d_up, o_halves, hidden, dy_halves, stacks):
            lhs = {0: u_halves, 1: o_halves, 2: u_halves, 3: u_halves, 4: hidden}[which]
            rhs = {0: d_qkv, 1: dy_halves, 2: d_gate, 3: d_up, 4: dy_halves}[which]
            name = ('wg_qkv', 'wg_out', 'wg_gate', 'wg_up', 'wg_down')[which]
            stacks[which] = wgrad(half, list(lhs), list(rhs), layer, n_layers, stacks[which], 256 if which == 1 else 512, name)

        d_hid1 = None
        for layer in range(n_layers):
            last = layer == n_layers - 1
            x_f32 = x_cur.astype(F32)
            u_loc = rms_scale(x_f32, norm_gain[layer]).astype(BF16)
            other = chip_swap(u_loc)
            u_near = jnp.concatenate([u_loc, core_swap(u_loc)], axis=0)
            near = project(layer, u_near, (d_hid1, 0) if last else None)
            if layer == 0:
                dy_core = core_swap(dy_loc)
                dy_near = jnp.concatenate([dy_loc, dy_core], axis=0)
                d_attn1_n = dot_t(dy_near, w_out[n_layers - 1]).astype(BF16)
                near[0], near[1], d_attn1_n, other = barrier(near[0], near[1], d_attn1_n, other)
            else:
                near[0], near[1], other = barrier(near[0], near[1], other)
            u_far = jnp.concatenate([other, core_swap(other)], axis=0)
            if layer == 0:
                dy_start, u_far = barrier(dy_loc, u_far)
                dy_other = chip_swap(dy_start)
            far = project(layer, u_far, (d_hid1, 1) if last else None)
            rot_qkv, o_n, o_f, lse = attn_fwd(base, near[0], far[0], cos_tab, sin_tab)
            saved.append({'x': x_cur, 'u': u_loc, 'rot': rot_qkv, 'o': ((o_n, 0), (o_f, 0)), 'lse': lse, 'gate': (near[1], far[1]), 'up': (near[2], far[2])})
            if last:
                break
            split_outs = [(rows, F32)] * 2
            far_keep, far_send = fused_mm('out_far', half, [(o_f, 0), (far[3], 0)], [w_out, w_down], False, layer, 512, [], split_sum_epilogue, split_outs)
            far_recv = core_swap(far_send)
            if layer == 0:
                dy_full = jnp.concatenate([dy_near, dy_other, core_swap(dy_other)], axis=0)
                dy_full, far_keep = barrier(dy_full, far_keep)
                d_attn1_f = dot_t(dy_full[half:], w_out[n_layers - 1]).astype(BF16)
                far_recv, d_attn1_f = barrier(far_recv, d_attn1_f)
            far_sum = far_keep + far_recv
            from_far = chip_swap(far_sum)
            o_n, near[3], far_sum = barrier(o_n, near[3], far_sum)
            near_keep, near_send = fused_mm('out_near', half, [(o_n, 0), (near[3], 0)], [w_out, w_down], False, layer, 512, [], split_sum_epilogue, split_outs)
            near_recv = core_swap(near_send)
            mid_sum = near_keep + near_recv
            x_sum = x_f32 + mid_sum
            d_hid1 = dot_t(dy_full, w_down[n_layers - 1]).astype(BF16)
            x_sum, d_hid1, from_far = barrier(x_sum, d_hid1, from_far)
            x_cur = (x_sum + from_far).astype(BF16)
        u_halves = ((u_near, 0), (u_far, 0))
        grad_cur = dy_loc
        stacks = [None] * 5
        gain_grads = [None] * n_layers
        for layer in reversed(range(n_layers)):
            kept = saved[layer]
            (gate_n, gate_f), (up_n, up_f) = kept['gate'], kept['up']
            if layer == n_layers - 1:
                dy_halves = ((dy_full, 0), (dy_full, 1))
                d_attn = ((d_attn1_n, 0), (d_attn1_f, 0))
            else:
                dy_near = jnp.concatenate([grad_cur, core_swap(grad_cur)], axis=0)
                dy_other = chip_swap(grad_cur)
                d_attn_near = dot_t(dy_near, w_out[layer]).astype(BF16)
            if layer == n_layers - 1:
                back_n, back_f = near[1:], far[1:]
            else:
                back_n = mlp_back(layer, half, dy_near, gate_n, up_n)
                stacks[4], back_n[0], dy_other = barrier(stacks[4], back_n[0], dy_other)
                dy_far = jnp.concatenate([dy_other, core_swap(dy_other)], axis=0)
                dy_halves = ((dy_near, 0), (dy_far, 0))
                d_attn_far = dot_t(dy_far, w_out[layer]).astype(BF16)
                d_attn = ((d_attn_near, 0), (d_attn_far, 0))
                back_f = mlp_back(layer, half, dy_far, gate_f, up_f)
                u_start, stacks[0], stacks[2], stacks[3], dy_other = barrier(kept['u'], stacks[0], stacks[2], stacks[3], dy_other)
                u_other = chip_swap(u_start)
                u_near = jnp.concatenate([u_start, core_swap(u_start)], axis=0)
                u_far = jnp.concatenate([u_other, core_swap(u_other)], axis=0)
                u_halves = ((u_near, 0), (u_far, 0))
            hidden, d_gate, d_up = [((back_n[idx], 0), (back_f[idx], 0)) for idx in range(3)]
            qkv_n, qkv_f = attn_bwd(base, kept['rot'], kept['lse'], d_attn, cos_tab, sin_tab)
            d_qkv = ((qkv_n, 0), (qkv_f, 0))
            w_args = (layer, u_halves, d_qkv, d_gate, d_up, kept['o'], hidden, dy_halves, stacks)

            def dgrad(side, name):
                return fused_mm(name, half, [d_qkv[side], d_gate[side], d_up[side]], [w_qkv, w_gate, w_up], True, layer, 512, [], split_sum_epilogue, [(rows, F32)] * 2)

            far_keep, far_send = dgrad(1, 'dgrad_far')
            far_recv = core_swap(far_send)
            wgrads(1, *w_args)
            stacks[1], far_recv = barrier(stacks[1], far_recv)
            far_sum = far_keep + far_recv
            from_far = chip_swap(far_sum)
            qkv_n, far_sum = barrier(qkv_n, far_sum)
            d_qkv = ((qkv_n, 0), (qkv_f, 0))
            near_keep, near_send = dgrad(0, 'dgrad_near')
            near_recv = core_swap(near_send)
            w_args = (layer, u_halves, d_qkv, d_gate, d_up, kept['o'], hidden, dy_halves, stacks)
            wgrads(0, *w_args)
            wgrads(2, *w_args)
            wgrads(3, *w_args)
            if layer == 0:
                wgrads(4, *w_args)
                stacks[4], from_far = barrier(stacks[4], from_far)
            stacks[0], stacks[2], stacks[3], from_far = barrier(stacks[0], stacks[2], stacks[3], from_far)
            d_normed = (near_keep + near_recv + from_far).astype(BF16)
            norm_pull = jax.vjp(rms_scale, kept['x'].astype(F32), norm_gain[layer])[1]
            d_x_norm, gain_grads[layer] = norm_pull(d_normed.astype(F32))
            grad_cur = (grad_cur.astype(F32) + d_x_norm).astype(BF16)
            if layer != 0:
                dy_halves = tuple(dy_halves)
                hid_n, hid_f, grad_tie = barrier(back_n[0], back_f[0], grad_cur)
                grad_cur = grad_tie
                w_args = (layer, u_halves, d_qkv, d_gate, d_up, kept['o'], ((hid_n, 0), (hid_f, 0)), dy_halves, stacks)
                wgrads(4, *w_args)
        gain = jnp.stack(gain_grads)
        gain = gain + core_swap(gain)
        gain = gain + chip_swap(gain)
        return (grad_cur, gain, stacks[0], stacks[1], stacks[2], stacks[3], stacks[4])

    return jax.shard_map(device_program, mesh=mesh, in_specs=(row_spec, row_spec, P(None, None), col_spec, inner_spec, col_spec, col_spec, inner_spec), out_specs=(row_spec, P('dp', None), P('dp', None, 'tp'), P('dp', 'tp', None), P('dp', None, 'tp'), P('dp', None, 'tp'), P('dp', 'tp', None)), check_vma=False)
```

```python
import jax
import jax.numpy as jnp
from jax import lax
from jax.experimental import pallas as pl
from jax.experimental.pallas import tpu as pltpu
from jax.sharding import PartitionSpec as P


HEAD_DIM = 128
NORM_EPS = 1e-5
ROPE_BASE = 10000.0
BF16 = jnp.bfloat16
F32 = jnp.float32
GROUP = 3
SCALE = HEAD_DIM ** -0.5
CORE_PAIRS = [(0, 1), (1, 0), (2, 3), (3, 2)]
CHIP_PAIRS = [(0, 2), (2, 0), (1, 3), (3, 1)]
VMEM_LIMIT = 40 << 20
MM_VMEM = 28 << 20
WG_VMEM = 36 << 20


def core_swap(values):
    return lax.ppermute(values, 'tp', CORE_PAIRS)


def chip_swap(values):
    return lax.ppermute(values, 'tp', CHIP_PAIRS)


def barrier(*values):
    return lax.optimization_barrier(values)


def rope_tables(seq_len):
    half_dim = HEAD_DIM // 2
    freqs = ROPE_BASE ** (-2.0 * jnp.arange(half_dim, dtype=F32) / HEAD_DIM)
    angles = jnp.arange(seq_len, dtype=F32)[:, None] * freqs[None, :]
    cos_tab, sin_tab = jnp.cos(angles), jnp.sin(angles)
    return jnp.concatenate([cos_tab, cos_tab], axis=1), jnp.concatenate([-sin_tab, sin_tab], axis=1)


def rms_scale(x_f32, gain_row):
    inv_rms = lax.rsqrt(jnp.mean(x_f32 * x_f32, axis=-1, keepdims=True) + NORM_EPS)
    return x_f32 * inv_rms * gain_row


def gated(gate_f32, up_f32):
    return jax.nn.silu(gate_f32) * up_f32


def dot(lhs, rhs):
    return jnp.dot(lhs, rhs, preferred_element_type=F32)


def dot_t(lhs, rhs):
    return lax.dot_general(lhs, rhs, (((1,), (1,)), ((), ())), preferred_element_type=F32)


def dot_lt(lhs, rhs):
    return lax.dot_general(lhs, rhs, (((0,), (0,)), ((), ())), preferred_element_type=F32)


def attn_fwd_kernel(base_ref, qn_ref, qf_ref, cos_ref, sin_ref, rq_ref, on_ref, of_ref, lse_ref, o_scr):
    rows = qn_ref.shape[0] // 2
    kcol, vcol = GROUP * HEAD_DIM, (GROUP + 1) * HEAD_DIM
    for k in range(4):
        src = qn_ref if k < 2 else qf_ref
        local = slice((k % 2) * rows, (k % 2 + 1) * rows)
        where = pl.ds(pl.multiple_of(base_ref[k] * rows, rows), rows)
        cos_tab, sin_tab = cos_ref[where, :], sin_ref[where, :]
        for h in range(GROUP + 1):
            cols = slice(h * HEAD_DIM, (h + 1) * HEAD_DIM)
            vals = src[local, cols].astype(F32)
            rq_ref[where, cols] = (vals * cos_tab + pltpu.roll(vals, HEAD_DIM // 2, 1) * sin_tab).astype(BF16)
        rq_ref[where, vcol:] = src[local, vcol:]
    causal = lax.broadcasted_iota(jnp.int32, (rows, rows), 0) >= lax.broadcasted_iota(jnp.int32, (rows, rows), 1)
    for i in range(4):
        width = (i + 1) * rows
        keys, vals = rq_ref[0:width, kcol:vcol], rq_ref[0:width, vcol:]
        for h in range(GROUP):
            query = rq_ref[i * rows:width, h * HEAD_DIM:(h + 1) * HEAD_DIM]
            scores = dot_t(query, keys) * SCALE
            diag = jnp.where(causal, scores[:, i * rows:], -1e30)
            scores = diag if i == 0 else jnp.concatenate([scores[:, :i * rows], diag], axis=1)
            row_max = jnp.max(scores, axis=1, keepdims=True)
            weights = jnp.exp(scores - row_max)
            total = jnp.sum(weights, axis=1, keepdims=True)
            prob = (weights * (1.0 / total)).astype(BF16)
            o_scr[i * rows:width, h * HEAD_DIM:(h + 1) * HEAD_DIM] = dot(prob, vals).astype(BF16)
            lse = jnp.broadcast_to(row_max + jnp.log(total), (rows, HEAD_DIM))
            lse_ref[0, h:h + 1, i * rows:width] = jnp.transpose(lse)[0:1, :]
    for k in range(4):
        dst = on_ref if k < 2 else of_ref
        dst[(k % 2) * rows:(k % 2 + 1) * rows, :] = o_scr[pl.ds(pl.multiple_of(base_ref[k] * rows, rows), rows), :]


def attn_fwd(base, qkv_n, qkv_f, cos_tab, sin_tab):
    half, width = cos_tab.shape[0] // 2, qkv_n.shape[1]
    cols = (GROUP + 2) * HEAD_DIM
    groups = width // cols
    seq_len = 2 * half
    smem = pl.BlockSpec(memory_space=pltpu.SMEM)
    tab = pl.BlockSpec((seq_len, HEAD_DIM), lambda j: (0, 0))
    half_in = pl.BlockSpec((half, cols), lambda j: (0, j))
    half_out = pl.BlockSpec((half, GROUP * HEAD_DIM), lambda j: (0, j))
    return pl.pallas_call(
        attn_fwd_kernel, grid=(groups,), name='attn_fwd',
        in_specs=[smem, half_in, half_in, tab, tab],
        out_specs=[pl.BlockSpec((seq_len, cols), lambda j: (0, j)), half_out, half_out, pl.BlockSpec((1, 8, seq_len), lambda j: (j, 0, 0))],
        out_shape=[out_struct((seq_len, width), BF16, True)] + [jax.ShapeDtypeStruct((half, groups * GROUP * HEAD_DIM), BF16)] * 2 + [jax.ShapeDtypeStruct((groups, 8, seq_len), F32)],
        scratch_shapes=[pltpu.VMEM((seq_len, GROUP * HEAD_DIM), BF16)],
        cost_estimate=pl.CostEstimate(flops=8 * 10 ** 9, bytes_accessed=8 * 10 ** 6, transcendentals=4 * 10 ** 6),
        compiler_params=pltpu.CompilerParams(vmem_limit_bytes=VMEM_LIMIT),
    )(base, qkv_n, qkv_f, cos_tab, sin_tab)


def attn_bwd_kernel(base_ref, rq_ref, lse_ref, dn_ref, df_ref, cos_ref, sin_ref, gn_ref, gf_ref, do_scr, dq_scr, dk_scr, dv_scr):
    rows = dn_ref.shape[0] // 2
    kcol, vcol = GROUP * HEAD_DIM, (GROUP + 1) * HEAD_DIM
    for k in range(4):
        src = dn_ref if k < 2 else df_ref
        do_scr[pl.ds(pl.multiple_of(base_ref[k] * rows, rows), rows), :] = src[(k % 2) * rows:(k % 2 + 1) * rows, :]
    dk_scr[...] = jnp.zeros_like(dk_scr)
    dv_scr[...] = jnp.zeros_like(dv_scr)
    causal = lax.broadcasted_iota(jnp.int32, (rows, rows), 1) >= lax.broadcasted_iota(jnp.int32, (rows, rows), 0)
    for i in range(4):
        width = (i + 1) * rows
        keys, vals = rq_ref[0:width, kcol:vcol], rq_ref[0:width, vcol:]
        for h in range(GROUP):
            cols = slice(h * HEAD_DIM, (h + 1) * HEAD_DIM)
            query, d_o = rq_ref[i * rows:width, cols], do_scr[i * rows:width, cols]
            scores = dot_t(keys, query) * SCALE
            diag = jnp.where(causal, scores[i * rows:, :], -1e30)
            scores = diag if i == 0 else jnp.concatenate([scores[:i * rows, :], diag], axis=0)
            prob = jnp.exp(scores - lse_ref[0, h:h + 1, i * rows:width])
            d_prob = dot_t(vals, d_o).astype(BF16).astype(F32)
            delta = jnp.sum(prob * d_prob, axis=0, keepdims=True)
            d_scores = (prob * (d_prob - delta) * SCALE).astype(BF16)
            dv_scr[0:width, :] += dot(prob.astype(BF16), d_o)
            dk_scr[0:width, :] += dot(d_scores, query)
            dq_scr[i * rows:width, cols] = dot_lt(d_scores, keys).astype(BF16)
    for k in range(4):
        dst = gn_ref if k < 2 else gf_ref
        local = slice((k % 2) * rows, (k % 2 + 1) * rows)
        where = pl.ds(pl.multiple_of(base_ref[k] * rows, rows), rows)
        cos_tab, sin_tab = cos_ref[where, :], sin_ref[where, :]
        for h in range(GROUP + 1):
            cols = slice(h * HEAD_DIM, (h + 1) * HEAD_DIM)
            vals = dq_scr[where, cols].astype(F32) if h < GROUP else dk_scr[where, :].astype(BF16).astype(F32)
            dst[local, cols] = (vals * cos_tab - pltpu.roll(vals, HEAD_DIM // 2, 1) * sin_tab).astype(BF16)
        dst[local, vcol:] = dv_scr[where, :].astype(BF16)


def attn_bwd(base, rot_qkv, lse, d_halves, cos_tab, sin_tab):
    seq_len, width = rot_qkv.shape
    half = seq_len // 2
    cols = (GROUP + 2) * HEAD_DIM
    groups = width // cols
    smem = pl.BlockSpec(memory_space=pltpu.SMEM)
    tab = pl.BlockSpec((seq_len, HEAD_DIM), lambda j: (0, 0))
    halves_in = [pl.BlockSpec((half, GROUP * HEAD_DIM), lambda j, r=r: (r, j)) for _, r in d_halves]
    half_out = pl.BlockSpec((half, cols), lambda j: (0, j))
    return pl.pallas_call(
        attn_bwd_kernel, grid=(groups,), name='attn_bwd',
        in_specs=[smem, pl.BlockSpec((seq_len, cols), lambda j: (0, j)), pl.BlockSpec((1, 8, seq_len), lambda j: (j, 0, 0)), *halves_in, tab, tab],
        out_specs=[half_out, half_out],
        out_shape=[jax.ShapeDtypeStruct((half, width), BF16)] * 2,
        scratch_shapes=[pltpu.VMEM((seq_len, GROUP * HEAD_DIM), BF16)] * 2 + [pltpu.VMEM((seq_len, HEAD_DIM), F32)] * 2,
        cost_estimate=pl.CostEstimate(flops=20 * 10 ** 9, bytes_accessed=8 * 10 ** 6, transcendentals=4 * 10 ** 6),
        compiler_params=pltpu.CompilerParams(vmem_limit_bytes=VMEM_LIMIT),
    )(base, rot_qkv, lse, d_halves[0][0], d_halves[1][0], cos_tab, sin_tab)


def wgrad_kernel(an_ref, af_ref, bn_ref, bf_ref, *rest):
    out_ref = rest[-1]
    out_ref[0] = (dot_lt(an_ref[...], bn_ref[...]) + dot_lt(af_ref[...], bf_ref[...])).astype(BF16)


def wgrad(half, lhs, rhs, layer_idx, n_layers, stacked, block_rows):
    m_dim, n_dim = lhs[0][0].shape[1], rhs[0][0].shape[1]
    in_specs = [pl.BlockSpec((half, block_rows), lambda m, r=r: (r, m)) for _, r in lhs]
    in_specs += [pl.BlockSpec((half, n_dim), lambda m, r=r: (r, 0)) for _, r in rhs]
    args = [arr for arr, _ in lhs + rhs]
    aliases = {}
    if stacked is not None:
        in_specs.append(pl.BlockSpec(memory_space=pl.ANY))
        args.append(stacked)
        aliases = {4: 0}
    return pl.pallas_call(
        wgrad_kernel, grid=(m_dim // block_rows,), in_specs=in_specs,
        out_specs=pl.BlockSpec((1, block_rows, n_dim), lambda m: (layer_idx, m, 0)),
        out_shape=jax.ShapeDtypeStruct((n_layers, m_dim, n_dim), BF16),
        input_output_aliases=aliases,
        cost_estimate=pl.CostEstimate(flops=4 * half * m_dim * n_dim, bytes_accessed=2 * (m_dim * n_dim + 2 * half * (m_dim + n_dim)), transcendentals=0),
        compiler_params=pltpu.CompilerParams(vmem_limit_bytes=WG_VMEM),
    )(*args)


def out_struct(shape, dtype, in_hbm=False):
    return pltpu.HBM(shape, dtype) if in_hbm else jax.ShapeDtypeStruct(shape, dtype)


def fused_mm(rows, xs, ws, trans, layer, block, extras, epilogue, outs, first=0, steps=None):
    steps = (ws[0].shape[1] if trans else ws[0].shape[2]) // block if steps is None else steps
    n_dim = steps * block
    n_x, n_e = len(xs), len(extras)

    def kernel(*refs):
        accs = [(dot_t if trans else dot)(refs[i][...], refs[n_x + i][0]) for i in range(n_x)]
        results = epilogue(accs, [ref[...] for ref in refs[2 * n_x:2 * n_x + n_e]])
        for ref, val in zip(refs[2 * n_x + n_e:], results):
            ref[...] = val.astype(ref.dtype)

    in_specs = [pl.BlockSpec((rows, x.shape[1]), lambda n, r=r: (r, 0)) for x, r in xs]
    if trans:
        in_specs += [pl.BlockSpec((1, block, w.shape[2]), lambda n: (layer, n + first, 0)) for w in ws]
    else:
        in_specs += [pl.BlockSpec((1, w.shape[1], block), lambda n: (layer, 0, n + first)) for w in ws]
    in_specs += [pl.BlockSpec((rows, block), lambda n, r=r: (r, n)) for _, r in extras]
    depth = sum(x.shape[1] for x, _ in xs)
    return list(pl.pallas_call(
        kernel, grid=(steps,), in_specs=in_specs,
        out_specs=[pl.BlockSpec((r, block), lambda n: (0, n)) for r, *_ in outs],
        out_shape=[out_struct((r, n_dim), *rest) for r, *rest in outs],
        cost_estimate=pl.CostEstimate(flops=2 * rows * depth * n_dim, bytes_accessed=2 * depth * (rows + n_dim) + 4 * rows * n_dim, transcendentals=0),
        compiler_params=pltpu.CompilerParams(vmem_limit_bytes=MM_VMEM),
    )(*[x for x, _ in xs], *ws, *[e for e, _ in extras]))


def gate_up_epilogue(accs, extras):
    gate, up = accs[0].astype(BF16), accs[1].astype(BF16)
    return gate, up, gated(gate.astype(F32), up.astype(F32))


def gate_up_back_epilogue(accs, extras):
    gate, up = accs[0].astype(BF16).astype(F32), accs[1].astype(BF16).astype(F32)
    hidden, pull = jax.vjp(gated, gate, up)
    return (hidden,) + pull(extras[0].astype(F32))


def split_sum_epilogue(accs, extras):
    total = sum(accs[1:], accs[0])
    rows = total.shape[0] // 2
    return total[:rows], total[rows:]


def mlp_back_epilogue(accs, extras):
    d_hid = accs[0].astype(BF16).astype(F32)
    gate, up = extras[0].astype(F32), extras[1].astype(F32)
    hidden, pull = jax.vjp(gated, gate, up)
    return (hidden,) + pull(d_hid)


def solution(mesh):
    row_spec = P(('dp', 'tp'), None)
    col_spec = P(None, None, 'tp')
    inner_spec = P(None, 'tp', None)

    def device_program(x_loc, dy_loc, norm_gain, w_qkv, w_out, w_gate, w_up, w_down):
        n_layers = w_qkv.shape[0]
        rows = x_loc.shape[0]
        half = 2 * rows
        rank = lax.axis_index('tp')
        base = jnp.bitwise_xor(jnp.arange(4, dtype=jnp.int32), rank.astype(jnp.int32))
        cos_tab, sin_tab = rope_tables(4 * rows)
        saved = []
        x_cur = x_loc

        def project(layer, u_half, d_hid):
            qkv = dot(u_half, w_qkv[layer]).astype(BF16)
            extras = [] if d_hid is None else [(d_hid, 0)]
            epilogue = gate_up_epilogue if d_hid is None else gate_up_back_epilogue
            return [qkv] + fused_mm(half, [(u_half, 0)] * 2, [w_gate, w_up], False, layer, 256, extras, epilogue, [(half, BF16, True)] * 2 + [(half, BF16, d_hid is not None)])

        def mlp_back(layer, n_rows, dy_half, gate_half, up_half):
            return fused_mm(n_rows, [(dy_half, 0)], [w_down], True, layer, 256, [(gate_half, 0), (up_half, 0)], mlp_back_epilogue, [(n_rows, BF16)] * 3)

        def wgrads(which, layer, u_halves, d_qkv, d_gate, d_up, o_halves, hidden, dy_halves, stacks):
            lhs = {0: u_halves, 1: o_halves, 2: u_halves, 3: u_halves, 4: hidden}[which]
            rhs = {0: d_qkv, 1: dy_halves, 2: d_gate, 3: d_up, 4: dy_halves}[which]
            stacks[which] = wgrad(half, list(lhs), list(rhs), layer, n_layers, stacks[which], 256 if which == 1 else 512)

        d_hid1 = dy_far = None
        for layer in range(n_layers):
            last = layer == n_layers - 1
            x_f32 = x_cur.astype(F32)
            u_loc = rms_scale(x_f32, norm_gain[layer]).astype(BF16)
            other = chip_swap(u_loc)
            u_near = jnp.concatenate([u_loc, core_swap(u_loc)], axis=0)
            near = project(layer, u_near, d_hid1[0] if last else None)
            if layer == 0:
                dy_core = core_swap(dy_loc)
                dy_near = jnp.concatenate([dy_loc, dy_core], axis=0)
                d_attn1_n = dot_t(dy_near, w_out[n_layers - 1]).astype(BF16)
                near[0], near[1], d_attn1_n, other = barrier(near[0], near[1], d_attn1_n, other)
            else:
                near[0], near[1], other = barrier(near[0], near[1], other)
            u_far = jnp.concatenate([other, core_swap(other)], axis=0)
            if layer == 0:
                dy_start, u_far = barrier(dy_loc, u_far)
                dy_other = chip_swap(dy_start)
            far = project(layer, u_far, d_hid1[1] if last else None)
            rot_qkv, o_n, o_f, lse = attn_fwd(base, near[0], far[0], cos_tab, sin_tab)
            saved.append({'x': x_cur, 'u': u_loc, 'rot': rot_qkv, 'o': ((o_n, 0), (o_f, 0)), 'lse': lse, 'gate': (near[1], far[1]), 'up': (near[2], far[2])})
            if last:
                break
            split_outs = [(rows, F32)] * 2
            n_cols = x_f32.shape[1] // 512 // 2

            def out_far(o_half, first):
                return fused_mm(half, [(o_half, 0), (far[3], 0)], [w_out, w_down], False, layer, 512, [], split_sum_epilogue, split_outs, first, n_cols)

            keep_a, send_a = out_far(o_f, 0)
            recv_a = core_swap(send_a)
            o_f, send_a = barrier(o_f, send_a)
            keep_b, send_b = out_far(o_f, n_cols)
            recv_b = core_swap(send_b)
            recv_a, keep_b = barrier(recv_a, keep_b)
            sum_a = keep_a + recv_a
            far_a = chip_swap(sum_a)
            o_n, near[3], sum_a = barrier(o_n, near[3], sum_a)
            near_keep, near_send = fused_mm(half, [(o_n, 0), (near[3], 0)], [w_out, w_down], False, layer, 512, [], split_sum_epilogue, split_outs)
            near_recv = core_swap(near_send)
            recv_b, near_keep = barrier(recv_b, near_keep)
            sum_b = keep_b + recv_b
            far_b = chip_swap(sum_b)
            if layer == 0:
                dy_near, dy_other, sum_b = barrier(dy_near, dy_other, sum_b)
                dy_far = jnp.concatenate([dy_other, core_swap(dy_other)], axis=0)
                d_attn1_f = dot_t(dy_far, w_out[n_layers - 1]).astype(BF16)
                d_hid1 = [dot_t(dy_half, w_down[n_layers - 1]).astype(BF16) for dy_half in (dy_near, dy_far)]
            x_sum = x_f32 + (near_keep + near_recv)
            x_sum, d_hid1[0], d_hid1[1], d_attn1_f, far_a, far_b = barrier(x_sum, d_hid1[0], d_hid1[1], d_attn1_f, far_a, far_b)
            x_cur = (x_sum + jnp.concatenate([far_a, far_b], axis=1)).astype(BF16)
        u_halves = ((u_near, 0), (u_far, 0))
        grad_cur = dy_loc
        stacks = [None] * 5
        gain_grads = [None] * n_layers
        for layer in reversed(range(n_layers)):
            kept = saved[layer]
            (gate_n, gate_f), (up_n, up_f) = kept['gate'], kept['up']
            if layer == n_layers - 1:
                dy_halves = ((dy_near, 0), (dy_far, 0))
                d_attn = ((d_attn1_n, 0), (d_attn1_f, 0))
            else:
                dy_near = jnp.concatenate([grad_cur, core_swap(grad_cur)], axis=0)
                dy_other = chip_swap(grad_cur)
                d_attn_near = dot_t(dy_near, w_out[layer]).astype(BF16)
            if layer == n_layers - 1:
                back_n, back_f = near[1:], far[1:]
            else:
                back_n = mlp_back(layer, half, dy_near, gate_n, up_n)
                stacks[4], back_n[0], dy_other = barrier(stacks[4], back_n[0], dy_other)
                dy_far = jnp.concatenate([dy_other, core_swap(dy_other)], axis=0)
                dy_halves = ((dy_near, 0), (dy_far, 0))
                d_attn_far = dot_t(dy_far, w_out[layer]).astype(BF16)
                d_attn = ((d_attn_near, 0), (d_attn_far, 0))
                back_f = mlp_back(layer, half, dy_far, gate_f, up_f)
                u_start, stacks[0], stacks[2], stacks[3], dy_other = barrier(kept['u'], stacks[0], stacks[2], stacks[3], dy_other)
                u_other = chip_swap(u_start)
                u_near = jnp.concatenate([u_start, core_swap(u_start)], axis=0)
                u_far = jnp.concatenate([u_other, core_swap(u_other)], axis=0)
                u_halves = ((u_near, 0), (u_far, 0))
            hidden, d_gate, d_up = [((back_n[idx], 0), (back_f[idx], 0)) for idx in range(3)]
            qkv_n, qkv_f = attn_bwd(base, kept['rot'], kept['lse'], d_attn, cos_tab, sin_tab)
            d_qkv = ((qkv_n, 0), (qkv_f, 0))
            w_args = (layer, u_halves, d_qkv, d_gate, d_up, kept['o'], hidden, dy_halves, stacks)

            def dgrad(side):
                return fused_mm(half, [d_qkv[side], d_gate[side], d_up[side]], [w_qkv, w_gate, w_up], True, layer, 512, [], split_sum_epilogue, [(rows, F32)] * 2)

            far_keep, far_send = dgrad(1)
            far_recv = core_swap(far_send)
            wgrads(1, *w_args)
            stacks[1], far_recv = barrier(stacks[1], far_recv)
            far_sum = far_keep + far_recv
            from_far = chip_swap(far_sum)
            qkv_n, far_sum = barrier(qkv_n, far_sum)
            d_qkv = ((qkv_n, 0), (qkv_f, 0))
            near_keep, near_send = dgrad(0)
            near_recv = core_swap(near_send)
            w_args = (layer, u_halves, d_qkv, d_gate, d_up, kept['o'], hidden, dy_halves, stacks)
            wgrads(0, *w_args)
            wgrads(2, *w_args)
            wgrads(3, *w_args)
            if layer == 0:
                wgrads(4, *w_args)
                stacks[4], from_far = barrier(stacks[4], from_far)
            stacks[0], stacks[2], stacks[3], from_far = barrier(stacks[0], stacks[2], stacks[3], from_far)
            d_normed = (near_keep + near_recv + from_far).astype(BF16)
            norm_pull = jax.vjp(rms_scale, kept['x'].astype(F32), norm_gain[layer])[1]
            d_x_norm, gain_grads[layer] = norm_pull(d_normed.astype(F32))
            grad_cur = (grad_cur.astype(F32) + d_x_norm).astype(BF16)
            if layer != 0:
                dy_halves = tuple(dy_halves)
                hid_n, hid_f, grad_tie = barrier(back_n[0], back_f[0], grad_cur)
                grad_cur = grad_tie
                w_args = (layer, u_halves, d_qkv, d_gate, d_up, kept['o'], ((hid_n, 0), (hid_f, 0)), dy_halves, stacks)
                wgrads(4, *w_args)
        gain = jnp.stack(gain_grads)
        gain = gain + core_swap(gain)
        gain = gain + chip_swap(gain)
        return (grad_cur, gain, stacks[0], stacks[1], stacks[2], stacks[3], stacks[4])

    return jax.shard_map(device_program, mesh=mesh, in_specs=(row_spec, row_spec, P(None, None), col_spec, inner_spec, col_spec, col_spec, inner_spec), out_specs=(row_spec, P('dp', None), P('dp', None, 'tp'), P('dp', 'tp', None), P('dp', None, 'tp'), P('dp', None, 'tp'), P('dp', 'tp', None)), check_vma=False)
```

```python
import functools

import jax
import jax.numpy as jnp
from jax import lax
from jax.experimental import pallas as pl
from jax.experimental.pallas import tpu as pltpu
from jax.sharding import PartitionSpec as P


HEAD_DIM = 128
NORM_EPS = 1e-5
ROPE_BASE = 10000.0
BF16 = jnp.bfloat16
F32 = jnp.float32
GROUP = 3
SCALE = HEAD_DIM ** -0.5
CORE_PAIRS = [(0, 1), (1, 0), (2, 3), (3, 2)]
CHIP_PAIRS = [(0, 2), (2, 0), (1, 3), (3, 1)]
CROSS_PAIRS = [(0, 3), (3, 0), (1, 2), (2, 1)]
VMEM_LIMIT = 40 << 20
MM_VMEM = 28 << 20
WG_VMEM = 36 << 20


def core_swap(values):
    return lax.ppermute(values, 'tp', CORE_PAIRS)


def chip_swap(values):
    return lax.ppermute(values, 'tp', CHIP_PAIRS)


def barrier(*values):
    return lax.optimization_barrier(values)


def rope_tables(seq_len):
    half_dim = HEAD_DIM // 2
    freqs = ROPE_BASE ** (-2.0 * jnp.arange(half_dim, dtype=F32) / HEAD_DIM)
    angles = jnp.arange(seq_len, dtype=F32)[:, None] * freqs[None, :]
    cos_tab, sin_tab = jnp.cos(angles), jnp.sin(angles)
    return jnp.concatenate([cos_tab, cos_tab], axis=1), jnp.concatenate([-sin_tab, sin_tab], axis=1)


def rms_scale(x_f32, gain_row):
    inv_rms = lax.rsqrt(jnp.mean(x_f32 * x_f32, axis=-1, keepdims=True) + NORM_EPS)
    return x_f32 * inv_rms * gain_row


def gated(gate_f32, up_f32):
    return jax.nn.silu(gate_f32) * up_f32


def dot(lhs, rhs):
    return jnp.dot(lhs, rhs, preferred_element_type=F32)


def dot_t(lhs, rhs):
    return lax.dot_general(lhs, rhs, (((1,), (1,)), ((), ())), preferred_element_type=F32)


def dot_lt(lhs, rhs):
    return lax.dot_general(lhs, rhs, (((0,), (0,)), ((), ())), preferred_element_type=F32)


def norm_kernel(layer, x_ref, gain_ref, dy_ref, u_ref, dy_copy_ref):
    u_ref[...] = rms_scale(x_ref[...].astype(F32), gain_ref[layer:layer + 1, :]).astype(BF16)
    dy_copy_ref[...] = dy_ref[...]


def norm(x_loc, norm_gain, layer, dy_loc):
    rows, width = x_loc.shape
    block = pl.BlockSpec((rows // 4, width), lambda i: (i, 0))
    return pl.pallas_call(
        functools.partial(norm_kernel, layer), grid=(4,), name='norm',
        in_specs=[block, pl.BlockSpec(norm_gain.shape, lambda i: (0, 0)), block], out_specs=[block, block],
        out_shape=[jax.ShapeDtypeStruct((rows, width), BF16), pltpu.VMEM((rows, width), BF16)],
        cost_estimate=pl.CostEstimate(flops=6 * rows * width, bytes_accessed=4 * rows * width, transcendentals=rows),
        compiler_params=pltpu.CompilerParams(vmem_limit_bytes=16 << 20),
    )(x_loc, norm_gain, dy_loc)


def attn_fwd_kernel(base_ref, qn_ref, qf_ref, cos_ref, sin_ref, rq_ref, on_ref, of_ref, lse_ref, o_scr):
    rows = qn_ref.shape[0] // 2
    kcol, vcol = GROUP * HEAD_DIM, (GROUP + 1) * HEAD_DIM
    for k in range(4):
        src = qn_ref if k < 2 else qf_ref
        local = slice((k % 2) * rows, (k % 2 + 1) * rows)
        where = pl.ds(pl.multiple_of(base_ref[k] * rows, rows), rows)
        cos_tab, sin_tab = cos_ref[where, :], sin_ref[where, :]
        for h in range(GROUP + 1):
            cols = slice(h * HEAD_DIM, (h + 1) * HEAD_DIM)
            vals = src[local, cols].astype(F32)
            rq_ref[where, cols] = (vals * cos_tab + pltpu.roll(vals, HEAD_DIM // 2, 1) * sin_tab).astype(BF16)
        rq_ref[where, vcol:] = src[local, vcol:]
    causal = lax.broadcasted_iota(jnp.int32, (rows, rows), 0) >= lax.broadcasted_iota(jnp.int32, (rows, rows), 1)
    for i in range(4):
        width = (i + 1) * rows
        keys, vals = rq_ref[0:width, kcol:vcol], rq_ref[0:width, vcol:]
        for h in range(GROUP):
            query = rq_ref[i * rows:width, h * HEAD_DIM:(h + 1) * HEAD_DIM]
            scores = dot_t(query, keys) * SCALE
            diag = jnp.where(causal, scores[:, i * rows:], -1e30)
            scores = diag if i == 0 else jnp.concatenate([scores[:, :i * rows], diag], axis=1)
            row_max = jnp.max(scores, axis=1, keepdims=True)
            weights = jnp.exp(scores - row_max)
            total = jnp.sum(weights, axis=1, keepdims=True)
            prob = (weights * (1.0 / total)).astype(BF16)
            o_scr[i * rows:width, h * HEAD_DIM:(h + 1) * HEAD_DIM] = dot(prob, vals).astype(BF16)
            lse = jnp.broadcast_to(row_max + jnp.log(total), (rows, HEAD_DIM))
            lse_ref[0, h:h + 1, i * rows:width] = jnp.transpose(lse)[0:1, :]
    for k in range(4):
        dst = on_ref if k < 2 else of_ref
        dst[(k % 2) * rows:(k % 2 + 1) * rows, :] = o_scr[pl.ds(pl.multiple_of(base_ref[k] * rows, rows), rows), :]


def attn_fwd(base, qkv_n, qkv_f, cos_tab, sin_tab):
    half, width = cos_tab.shape[0] // 2, qkv_n.shape[1]
    cols = (GROUP + 2) * HEAD_DIM
    groups = width // cols
    seq_len = 2 * half
    smem = pl.BlockSpec(memory_space=pltpu.SMEM)
    tab = pl.BlockSpec((seq_len, HEAD_DIM), lambda j: (0, 0))
    half_in = pl.BlockSpec((half, cols), lambda j: (0, j))
    half_out = pl.BlockSpec((half, GROUP * HEAD_DIM), lambda j: (0, j))
    return pl.pallas_call(
        attn_fwd_kernel, grid=(groups,), name='attn_fwd',
        in_specs=[smem, half_in, half_in, tab, tab],
        out_specs=[pl.BlockSpec((seq_len, cols), lambda j: (0, j)), half_out, half_out, pl.BlockSpec((1, 8, seq_len), lambda j: (j, 0, 0))],
        out_shape=[out_struct((seq_len, width), BF16, True)] + [jax.ShapeDtypeStruct((half, groups * GROUP * HEAD_DIM), BF16)] * 2 + [jax.ShapeDtypeStruct((groups, 8, seq_len), F32)],
        scratch_shapes=[pltpu.VMEM((seq_len, GROUP * HEAD_DIM), BF16)],
        cost_estimate=pl.CostEstimate(flops=8 * 10 ** 9, bytes_accessed=8 * 10 ** 6, transcendentals=4 * 10 ** 6),
        compiler_params=pltpu.CompilerParams(vmem_limit_bytes=VMEM_LIMIT),
    )(base, qkv_n, qkv_f, cos_tab, sin_tab)


def attn_bwd_kernel(base_ref, rq_ref, lse_ref, dn_ref, df_ref, cos_ref, sin_ref, gn_ref, gf_ref, do_scr, dq_scr, dk_scr, dv_scr):
    rows = dn_ref.shape[0] // 2
    kcol, vcol = GROUP * HEAD_DIM, (GROUP + 1) * HEAD_DIM
    for k in range(4):
        src = dn_ref if k < 2 else df_ref
        do_scr[pl.ds(pl.multiple_of(base_ref[k] * rows, rows), rows), :] = src[(k % 2) * rows:(k % 2 + 1) * rows, :]
    dk_scr[...] = jnp.zeros_like(dk_scr)
    dv_scr[...] = jnp.zeros_like(dv_scr)
    causal = lax.broadcasted_iota(jnp.int32, (rows, rows), 1) >= lax.broadcasted_iota(jnp.int32, (rows, rows), 0)
    for i in range(4):
        width = (i + 1) * rows
        keys, vals = rq_ref[0:width, kcol:vcol], rq_ref[0:width, vcol:]
        for h in range(GROUP):
            cols = slice(h * HEAD_DIM, (h + 1) * HEAD_DIM)
            query, d_o = rq_ref[i * rows:width, cols], do_scr[i * rows:width, cols]
            scores = dot_t(keys, query) * SCALE
            diag = jnp.where(causal, scores[i * rows:, :], -1e30)
            scores = diag if i == 0 else jnp.concatenate([scores[:i * rows, :], diag], axis=0)
            prob = jnp.exp(scores - lse_ref[0, h:h + 1, i * rows:width])
            d_prob = dot_t(vals, d_o).astype(BF16).astype(F32)
            delta = jnp.sum(prob * d_prob, axis=0, keepdims=True)
            d_scores = (prob * (d_prob - delta) * SCALE).astype(BF16)
            dv_scr[0:width, :] += dot(prob.astype(BF16), d_o)
            dk_scr[0:width, :] += dot(d_scores, query)
            dq_scr[i * rows:width, cols] = dot_lt(d_scores, keys).astype(BF16)
    for k in range(4):
        dst = gn_ref if k < 2 else gf_ref
        local = slice((k % 2) * rows, (k % 2 + 1) * rows)
        where = pl.ds(pl.multiple_of(base_ref[k] * rows, rows), rows)
        cos_tab, sin_tab = cos_ref[where, :], sin_ref[where, :]
        for h in range(GROUP + 1):
            cols = slice(h * HEAD_DIM, (h + 1) * HEAD_DIM)
            vals = dq_scr[where, cols].astype(F32) if h < GROUP else dk_scr[where, :].astype(BF16).astype(F32)
            dst[local, cols] = (vals * cos_tab - pltpu.roll(vals, HEAD_DIM // 2, 1) * sin_tab).astype(BF16)
        dst[local, vcol:] = dv_scr[where, :].astype(BF16)


def attn_bwd(base, rot_qkv, lse, d_halves, cos_tab, sin_tab):
    seq_len, width = rot_qkv.shape
    half = seq_len // 2
    cols = (GROUP + 2) * HEAD_DIM
    groups = width // cols
    smem = pl.BlockSpec(memory_space=pltpu.SMEM)
    tab = pl.BlockSpec((seq_len, HEAD_DIM), lambda j: (0, 0))
    halves_in = [pl.BlockSpec((half, GROUP * HEAD_DIM), lambda j, r=r: (r, j)) for _, r in d_halves]
    half_out = pl.BlockSpec((half, cols), lambda j: (0, j))
    return pl.pallas_call(
        attn_bwd_kernel, grid=(groups,), name='attn_bwd',
        in_specs=[smem, pl.BlockSpec((seq_len, cols), lambda j: (0, j)), pl.BlockSpec((1, 8, seq_len), lambda j: (j, 0, 0)), *halves_in, tab, tab],
        out_specs=[half_out, half_out],
        out_shape=[jax.ShapeDtypeStruct((half, width), BF16)] * 2,
        scratch_shapes=[pltpu.VMEM((seq_len, GROUP * HEAD_DIM), BF16)] * 2 + [pltpu.VMEM((seq_len, HEAD_DIM), F32)] * 2,
        cost_estimate=pl.CostEstimate(flops=20 * 10 ** 9, bytes_accessed=8 * 10 ** 6, transcendentals=4 * 10 ** 6),
        compiler_params=pltpu.CompilerParams(vmem_limit_bytes=VMEM_LIMIT),
    )(base, rot_qkv, lse, d_halves[0][0], d_halves[1][0], cos_tab, sin_tab)


def mxu_passes(rows, tiles, emit):
    def body(*accs):
        for g, pair in enumerate(tiles):
            use = accs[2 * (g % (len(accs) // 2)):][:2]
            for step in range(max(len(t) for t in pair)):
                for q, tile in enumerate(pair):
                    lhs, rhs, transposed = tile[step]
                    pltpu.matmul_push_rhs(rhs(), staging_register=step % 2, mxu_index=q, transpose=transposed)
                    pltpu.matmul_acc_lhs(use[q], lhs(), load_staged_rhs=step % 2)
            emit(g, [pltpu.matmul_pop(use[q]) for q in range(2)])

    n_acc = 2 if rows <= 512 else 1
    pl.run_scoped(body, *[pltpu.ACC(q)((rows, 256), F32) for _ in range(n_acc) for q in range(2)])


def wgrad(lhs, rhs, layer_idx, n_layers, stacked, block_rows):
    m_dim, n_dim = lhs[0][0].shape[1], rhs[0][0].shape[1]
    n_l, n_r = len(lhs), len(rhs)
    depth = sum(rows for _, _, rows in lhs)

    def kernel(*refs):
        out_ref, t_scr = refs[-2:]
        row = 0
        for ref, (_, _, rows) in zip(refs, lhs):
            t_scr[:, row:row + rows] = jnp.transpose(ref[...])
            row += rows
        where = [(ref, k) for ref, (_, _, rows) in zip(refs[n_l:n_l + n_r], rhs) for k in range(0, rows, 256)]

        def passes(part, col):
            def one(k):
                ref, first = where[k]
                return lambda: t_scr[part, k * 256:(k + 1) * 256], lambda: ref[first:first + 256, col:col + 256], False

            return [one(k) for k in range(len(where))]

        whole = slice(0, block_rows)
        halves = [slice(0, block_rows // 2), slice(block_rows // 2, block_rows)]

        def emit(g, accs):
            for q in range(2):
                out_ref[0, :, g * 512 + q * 256:g * 512 + q * 256 + 256] = accs[q].astype(BF16)

        def emit_last(g, accs):
            for q in range(2):
                out_ref[0, halves[q], n_dim - 256:] = accs[q].astype(BF16)

        mxu_passes(block_rows, [[passes(whole, col), passes(whole, col + 256)] for col in range(0, n_dim - 511, 512)], emit)
        if n_dim % 512:
            mxu_passes(block_rows // 2, [[passes(half, n_dim - 256) for half in halves]], emit_last)

    in_specs = [pl.BlockSpec((rows, block_rows), lambda m, r=first // rows: (r, m)) for _, first, rows in lhs]
    in_specs += [pl.BlockSpec((rows, n_dim), lambda m, r=first // rows: (r, 0)) for _, first, rows in rhs]
    args = [piece[0] for piece in lhs + rhs]
    aliases = {}
    if stacked is not None:
        in_specs.append(pl.BlockSpec(memory_space=pl.ANY))
        aliases = {len(args): 0}
        args.append(stacked)
    return pl.pallas_call(
        kernel, grid=(m_dim // block_rows,), in_specs=in_specs,
        out_specs=pl.BlockSpec((1, block_rows, n_dim), lambda m: (layer_idx, m, 0)),
        out_shape=jax.ShapeDtypeStruct((n_layers, m_dim, n_dim), BF16),
        input_output_aliases=aliases,
        scratch_shapes=[pltpu.VMEM((block_rows, depth), BF16)],
        cost_estimate=pl.CostEstimate(flops=2 * depth * m_dim * n_dim, bytes_accessed=2 * (m_dim * n_dim + depth * (m_dim + n_dim)), transcendentals=0),
        compiler_params=pltpu.CompilerParams(vmem_limit_bytes=WG_VMEM),
    )(*args)


def out_struct(shape, dtype, in_hbm=False):
    return pltpu.HBM(shape, dtype) if in_hbm else jax.ShapeDtypeStruct(shape, dtype)


def fused_mm(rows, xs, ws, trans, layer, block, extras, epilogue, outs, first=0, steps=None):
    steps = (ws[0].shape[1] if trans else ws[0].shape[2]) // block if steps is None else steps
    n_dim = steps * block
    n_x, n_e = len(xs), len(extras)

    def kernel(*refs):
        accs = [(dot_t if trans else dot)(refs[i][...], refs[n_x + i][0]) for i in range(n_x)]
        results = epilogue(accs, [ref[...] for ref in refs[2 * n_x:2 * n_x + n_e]])
        for ref, val in zip(refs[2 * n_x + n_e:], results):
            ref[...] = val.astype(ref.dtype)

    in_specs = [pl.BlockSpec((rows, x.shape[1]), lambda n, r=r: (r, 0)) for x, r in xs]
    if trans:
        in_specs += [pl.BlockSpec((1, block, w.shape[2]), lambda n: (layer, n + first, 0)) for w in ws]
    else:
        in_specs += [pl.BlockSpec((1, w.shape[1], block), lambda n: (layer, 0, n + first)) for w in ws]
    in_specs += [pl.BlockSpec((rows, block), lambda n, r=r: (r, n)) for _, r in extras]
    depth = sum(x.shape[1] for x, _ in xs)
    return list(pl.pallas_call(
        kernel, grid=(steps,), in_specs=in_specs,
        out_specs=[pl.BlockSpec((r, block), lambda n: (0, n)) for r, *_ in outs],
        out_shape=[out_struct((r, n_dim), *rest) for r, *rest in outs],
        cost_estimate=pl.CostEstimate(flops=2 * rows * depth * n_dim, bytes_accessed=2 * depth * (rows + n_dim) + 4 * rows * n_dim, transcendentals=0),
        compiler_params=pltpu.CompilerParams(vmem_limit_bytes=MM_VMEM),
    )(*[x for x, _ in xs], *ws, *[e for e, _ in extras]))


def gate_up_epilogue(accs, extras):
    gate, up = accs[0].astype(BF16), accs[1].astype(BF16)
    return gate, up, gated(gate.astype(F32), up.astype(F32))


def gate_up_back_epilogue(accs, extras):
    gate, up = accs[0].astype(BF16).astype(F32), accs[1].astype(BF16).astype(F32)
    hidden, pull = jax.vjp(gated, gate, up)
    return (hidden,) + pull(extras[0].astype(F32))


def split_sum_epilogue(accs, extras):
    total = sum(accs[1:], accs[0])
    rows = total.shape[0] // 2
    return total[:rows], total[rows:]


def mlp_back_epilogue(accs, extras):
    d_hid = accs[0].astype(BF16).astype(F32)
    gate, up = extras[0].astype(F32), extras[1].astype(F32)
    hidden, pull = jax.vjp(gated, gate, up)
    return (hidden,) + pull(d_hid)


def solution(mesh):
    row_spec = P(('dp', 'tp'), None)
    col_spec = P(None, None, 'tp')
    inner_spec = P(None, 'tp', None)

    def device_program(x_loc, dy_loc, norm_gain, w_qkv, w_out, w_gate, w_up, w_down):
        n_layers = w_qkv.shape[0]
        rows = x_loc.shape[0]
        half = 2 * rows
        rank = lax.axis_index('tp')
        base = jnp.bitwise_xor(jnp.arange(4, dtype=jnp.int32), rank.astype(jnp.int32))
        cos_tab, sin_tab = rope_tables(4 * rows)
        saved = []
        x_cur = x_loc

        def project(layer, u_half, d_hid):
            qkv = dot(u_half, w_qkv[layer]).astype(BF16)
            extras = [] if d_hid is None else [(d_hid, 0)]
            epilogue = gate_up_epilogue if d_hid is None else gate_up_back_epilogue
            return [qkv] + fused_mm(half, [(u_half, 0)] * 2, [w_gate, w_up], False, layer, 256, extras, epilogue, [(half, BF16, True)] * 2 + [(half, BF16, d_hid is not None)])

        def mlp_back(layer, n_rows, dy_half, gate_half, up_half):
            return fused_mm(n_rows, [(dy_half, 0)], [w_down], True, layer, 512, [(gate_half, 0), (up_half, 0)], mlp_back_epilogue, [(n_rows, BF16, True)] * 3)

        def pieces(*arrays):
            return [(arr, 0, arr.shape[0]) for arr in arrays]

        def wgrads(which, layer, u_pieces, d_qkv, d_gate, d_up, o_halves, hidden, dy_halves, stacks):
            lhs = {0: u_pieces, 1: pieces(*o_halves), 2: u_pieces, 3: u_pieces, 4: pieces(*hidden)}[which]
            rhs = pieces(*{0: d_qkv, 1: dy_halves, 2: d_gate, 3: d_up, 4: dy_halves}[which])
            stacks[which] = wgrad(lhs, rhs, layer, n_layers, stacks[which], 256 if which == 1 else 512)

        d_hid1 = dy_far = None
        for layer in range(n_layers):
            last = layer == n_layers - 1
            x_f32 = x_cur.astype(F32)
            if layer == 0:
                u_loc, dy_vmem = norm(x_cur, norm_gain, layer, dy_loc)
            else:
                u_loc = rms_scale(x_f32, norm_gain[layer]).astype(BF16)
            other = chip_swap(u_loc)
            u_near = jnp.concatenate([u_loc, core_swap(u_loc)], axis=0)
            near = project(layer, u_near, d_hid1[0] if last else None)
            if layer == 0:
                dy_core = core_swap(dy_loc)
                dy_near = jnp.concatenate([dy_loc, dy_core], axis=0)
                d_attn1_n = dot_t(dy_near, w_out[n_layers - 1]).astype(BF16)
                near[0], near[1], d_attn1_n, other = barrier(near[0], near[1], d_attn1_n, other)
            else:
                near[0], near[1], other = barrier(near[0], near[1], other)
            u_far = jnp.concatenate([other, core_swap(other)], axis=0)
            if layer == 0:
                dy_start, u_far = barrier(dy_vmem, u_far)
                dy_other = chip_swap(dy_start)
            far = project(layer, u_far, d_hid1[1] if last else None)
            rot_qkv, o_n, o_f, lse = attn_fwd(base, near[0], far[0], cos_tab, sin_tab)
            saved.append({'x': x_cur, 'u': u_loc, 'rot': rot_qkv, 'o': (o_n, o_f), 'lse': lse, 'gate': (near[1], far[1]), 'up': (near[2], far[2])})
            if last:
                break
            split_outs = [(rows, F32)] * 2
            n_cols = x_f32.shape[1] // 512 // 2

            def out_far(o_half, first):
                return fused_mm(half, [(o_half, 0), (far[3], 0)], [w_out, w_down], False, layer, 512, [], split_sum_epilogue, split_outs, first, n_cols)

            keep_a, send_a = out_far(o_f, 0)
            recv_a = core_swap(send_a)
            o_f, send_a = barrier(o_f, send_a)
            keep_b, send_b = out_far(o_f, n_cols)
            recv_b = core_swap(send_b)
            recv_a, keep_b = barrier(recv_a, keep_b)
            sum_a = keep_a + recv_a
            far_a = chip_swap(sum_a)
            o_n, near[3], sum_a = barrier(o_n, near[3], sum_a)
            near_keep, near_send = fused_mm(half, [(o_n, 0), (near[3], 0)], [w_out, w_down], False, layer, 512, [], split_sum_epilogue, split_outs)
            near_recv = core_swap(near_send)
            recv_b, near_keep = barrier(recv_b, near_keep)
            sum_b = keep_b + recv_b
            far_b = chip_swap(sum_b)
            if layer == 0:
                dy_near, dy_other, sum_b = barrier(dy_near, dy_other, sum_b)
                dy_far = jnp.concatenate([dy_other, core_swap(dy_other)], axis=0)
                d_attn1_f = dot_t(dy_far, w_out[n_layers - 1]).astype(BF16)
                d_hid1 = [dot_t(dy_half, w_down[n_layers - 1]).astype(BF16) for dy_half in (dy_near, dy_far)]
            x_sum = x_f32 + (near_keep + near_recv)
            x_sum, d_hid1[0], d_hid1[1], d_attn1_f, far_a, far_b = barrier(x_sum, d_hid1[0], d_hid1[1], d_attn1_f, far_a, far_b)
            x_cur = (x_sum + jnp.concatenate([far_a, far_b], axis=1)).astype(BF16)
        u_pieces = pieces(u_near, u_far)
        grad_cur = dy_loc
        stacks = [None] * 5
        gain_grads = [None] * n_layers
        for layer in reversed(range(n_layers)):
            kept = saved[layer]
            (gate_n, gate_f), (up_n, up_f) = kept['gate'], kept['up']
            if layer == n_layers - 1:
                dy_halves = (dy_near, dy_far)
                d_attn = ((d_attn1_n, 0), (d_attn1_f, 0))
            else:
                dy_near = jnp.concatenate([grad_cur, core_swap(grad_cur)], axis=0)
                dy_other = chip_swap(grad_cur)
                d_attn_near = dot_t(dy_near, w_out[layer]).astype(BF16)
            if layer == n_layers - 1:
                back_n, back_f = near[1:], far[1:]
            else:
                back_n = mlp_back(layer, half, dy_near, gate_n, up_n)
                stacks[4], back_n[0], dy_other = barrier(stacks[4], back_n[0], dy_other)
                dy_far = jnp.concatenate([dy_other, core_swap(dy_other)], axis=0)
                dy_halves = (dy_near, dy_far)
                d_attn_far = dot_t(dy_far, w_out[layer]).astype(BF16)
                d_attn = ((d_attn_near, 0), (d_attn_far, 0))
                back_f = mlp_back(layer, half, dy_far, gate_f, up_f)
                u_start, stacks[0], stacks[2], stacks[3], dy_other = barrier(kept['u'], stacks[0], stacks[2], stacks[3], dy_other)
                u_other = chip_swap(u_start)
                u_pieces = pieces(u_start, core_swap(u_start), u_other, core_swap(u_other))
            hidden, d_gate, d_up = [(back_n[idx], back_f[idx]) for idx in range(3)]
            qkv_n, qkv_f = attn_bwd(base, kept['rot'], kept['lse'], d_attn, cos_tab, sin_tab)
            d_qkv = (qkv_n, qkv_f)
            w_args = (layer, u_pieces, d_qkv, d_gate, d_up, kept['o'], hidden, dy_halves, stacks)

            w_args = (layer, u_pieces, d_qkv, d_gate, d_up, kept['o'], hidden, dy_halves, stacks)

            def dgrad(side):
                return fused_mm(half, [(d_qkv[side], 0), (d_gate[side], 0), (d_up[side], 0)], [w_qkv, w_gate, w_up], True, layer, 512, [], split_sum_epilogue, [(rows, F32)] * 2)

            far_keep, far_send = dgrad(1)
            far_recv = core_swap(far_send)
            wgrads(1, *w_args)
            stacks[1], far_recv = barrier(stacks[1], far_recv)
            far_sum = far_keep + far_recv
            from_far = chip_swap(far_sum)
            qkv_n, hid_n, gate_n, up_n, far_sum = barrier(qkv_n, hidden[0], d_gate[0], d_up[0], far_sum)
            hidden, d_gate, d_up = (hid_n, hidden[1]), (gate_n, d_gate[1]), (up_n, d_up[1])
            d_qkv = (qkv_n, qkv_f)
            near_keep, near_send = dgrad(0)
            near_recv = core_swap(near_send)
            w_args = (layer, u_pieces, d_qkv, d_gate, d_up, kept['o'], hidden, dy_halves, stacks)
            wgrads(0, *w_args)
            wgrads(2, *w_args)
            wgrads(3, *w_args)
            if layer == 0:
                wgrads(4, *w_args)
                stacks[4], from_far = barrier(stacks[4], from_far)
            stacks[0], stacks[2], stacks[3], from_far = barrier(stacks[0], stacks[2], stacks[3], from_far)
            d_normed = (near_keep + near_recv + from_far).astype(BF16)
            norm_pull = jax.vjp(rms_scale, kept['x'].astype(F32), norm_gain[layer])[1]
            d_x_norm, gain_grads[layer] = norm_pull(d_normed.astype(F32))
            grad_cur = (grad_cur.astype(F32) + d_x_norm).astype(BF16)
            if layer != 0:
                hid_n, hid_f, grad_cur = barrier(hidden[0], hidden[1], grad_cur)
                w_args = (layer, u_pieces, d_qkv, d_gate, d_up, kept['o'], (hid_n, hid_f), dy_halves, stacks)
                wgrads(4, *w_args)
        gain = jnp.stack(gain_grads)
        gain = (gain + core_swap(gain)) + (chip_swap(gain) + lax.ppermute(gain, 'tp', CROSS_PAIRS))
        return (grad_cur, gain, stacks[0], stacks[1], stacks[2], stacks[3], stacks[4])

    return jax.shard_map(device_program, mesh=mesh, in_specs=(row_spec, row_spec, P(None, None), col_spec, inner_spec, col_spec, col_spec, inner_spec), out_specs=(row_spec, P('dp', None), P('dp', None, 'tp'), P('dp', 'tp', None), P('dp', None, 'tp'), P('dp', None, 'tp'), P('dp', 'tp', None)), check_vma=False)
```
